32 devices in a mesh: site: 2 (over core), rows: 2 (over x), cols: 8 (over z, y).
Axes of the slice: x: 2, y: 2, z: 4, core: 2. Of those that a mesh axis runs over, the one named last changes fastest.
Arguments:
- tracer: float32 [128, 256, 128], P(('site', 'rows'), 'cols'), parts along dimension 0, may hold values from 0.5 to 2
- flow_y: float32 [128, 256, 128], P(('site', 'rows'), 'cols'), parts along dimension 0, may hold values from -0.3 to 0.3
- flow_x: float32 [128, 256, 128], P(('site', 'rows'), 'cols'), parts along dimension 0, may hold values from -0.3 to 0.3
Outputs:
- scaled_field: float32 [128, 256, 128], P(('site', 'rows'), 'cols'), parts along dimension 0
- tracer_end: float32 [128, 256, 128], P(('site', 'rows'), 'cols'), parts along dimension 0
The draws below stay inside these ranges and needn't reach their ends.
There are 2 independent parts, one for each index of `site`. The reference program is written for one: setup_inputs(seed, part) draws one part's arguments, and reference() takes and returns one part's arrays. A program takes and returns all parts, laid end to end along the dimension named above; each array names one. Nothing has to cross between parts.
All inputs are finite; a program needn't handle non-finite values.
Results may differ from the reference program's by a relative error of at most 0.00002.
Values sent between devices are 32-bit elements; how exact they have to be, the bound alone decides.
A program may use at most 64 MiB of HBM per device.

```python
import jax
import jax.numpy as jnp
from jax import lax

GRID_Y = 64
GRID_X = 256
SPECIES = 128
STEPS = 6


def block_levels(rng, shape, cuts, low, top_value):
    def one(dim, parts):
        heights = jax.random.uniform(jax.random.fold_in(jax.random.fold_in(rng, 6), dim), (parts,), jnp.float32, low / len(cuts), top_value / len(cuts))
        return jnp.repeat(jnp.exp(heights), shape[dim] // parts).reshape((-1,) + (1,) * (len(shape) - dim - 1))

    factor_of = one(*cuts[0])
    for cut in cuts[1:]:
        factor_of = factor_of * one(*cut)
    return factor_of


def setup_inputs(seed: int = 0, part: int = 0) -> dict:
    streams_of = jax.random.split(jax.random.key(seed), 4)
    part_splits = jax.random.split(jax.random.fold_in(streams_of[3], part), 4)
    return {
        "tracer": jnp.clip(0.5 + 1.5 * jax.random.uniform(part_splits[0], (GRID_Y, GRID_X, SPECIES), jnp.float32) ** block_levels(part_splits[0], (GRID_Y, GRID_X, SPECIES), ((0, 2), (1, 8)), -0.2, 0.2), 0.5, 2.0),
        "flow_y": jnp.clip(jax.random.uniform(part_splits[1], (GRID_Y, GRID_X, SPECIES), jnp.float32, -0.3, 0.3) * block_levels(part_splits[1], (GRID_Y, GRID_X, SPECIES), ((0, 2), (1, 8)), -0.4, 0.0), -0.3, 0.3),
        "flow_x": jnp.clip(jax.random.uniform(part_splits[2], (GRID_Y, GRID_X, SPECIES), jnp.float32, -0.3, 0.3) * block_levels(part_splits[2], (GRID_Y, GRID_X, SPECIES), ((0, 2), (1, 8)), -0.4, 0.0), -0.3, 0.3),
    }


def strip_edges(values, dims):
    for dim in dims:
        values = lax.slice_in_dim(values, 1, values.shape[dim] - 1, axis=dim)
    return values

def neighbour(values, dim, start, dims):
    others = [other for other in dims if other != dim]
    values = strip_edges(values, others)
    return lax.slice_in_dim(values, start, start + values.shape[dim] - 2, axis=dim)

def one_step(padded, flow_y, flow_x):
    middle = strip_edges(padded, (0, 1))
    lower = [neighbour(padded, dim, 0, (0, 1)) for dim in (0, 1)]
    upper = [neighbour(padded, dim, 2, (0, 1)) for dim in (0, 1)]
    slopes = [above - below for above, below in zip(upper, lower)]
    smooth_rate = 0.05
    spread = lower[0] + upper[0] + lower[1] + upper[1] - 4.0 * middle
    return middle - flow_y * slopes[0] - flow_x * slopes[1] + smooth_rate * spread

def reference(tracer, flow_y, flow_x):
    for step in range(STEPS):
        tracer = one_step(jnp.pad(tracer, ((1, 1), (1, 1), (0, 0)), mode='constant'), flow_y, flow_x)
    line_mean = lax.optimization_barrier(jnp.mean(tracer, axis=1, keepdims=True))
    centred = tracer - line_mean
    line_variance = lax.optimization_barrier(jnp.mean(centred * centred, axis=1, keepdims=True))
    scaled_field = centred * lax.rsqrt(line_variance + 0.0001)
    return (scaled_field, tracer)
```

```python
import functools

import jax
import jax.numpy as jnp
from jax import lax
from jax.experimental import pallas as pl
from jax.experimental.pallas import tpu as pltpu
from jax.sharding import PartitionSpec as P

MESH = pl.DeviceIdType.MESH
DEPTHS = (3, 3)
PAD = 8
SIDES = tuple((dy, dx) for dy in (-1, 0, 1) for dx in (-1, 0, 1) if (dy, dx) != (0, 0))


def spans(side, depth, size, first):
    if side == 0:
        return pl.ds(0, size), pl.ds(first, size)
    if side < 0:
        return pl.ds(0, depth), pl.ds(first + size, depth)
    return pl.ds(size - depth, depth), pl.ds(first - depth, depth)


def kernel(rows, cols, by, bx, t_hbm, fy_hbm, fx_hbm, scaled_hbm, end_hbm,
           fields, ping, fy, fx, final, scaled, stats, gathered,
           load_sem, send_sem, recv_sem, stat_send, stat_recv, store_sem):
    row, col = lax.axis_index("rows"), lax.axis_index("cols")
    top = max(DEPTHS)

    def exists(dy, dx):
        ok = None
        for step, here, count in ((dy, row, rows), (dx, col, cols)):
            if step:
                inside = (here > 0) if step < 0 else (here < count - 1)
                ok = inside if ok is None else jnp.logical_and(ok, inside)
        return ok

    loads = [
        pltpu.make_async_copy(t_hbm, fields.at[0, pl.ds(top, by), pl.ds(PAD, bx)], load_sem.at[0]),
        pltpu.make_async_copy(fy_hbm, fy.at[pl.ds(top, by), pl.ds(PAD, bx)], load_sem.at[1]),
        pltpu.make_async_copy(fx_hbm, fx.at[pl.ds(top, by), pl.ds(PAD, bx)], load_sem.at[2]),
    ]
    for load in loads:
        load.start()

    barrier = pltpu.get_barrier_semaphore()

    @pl.loop(1, cols)
    def _(k):
        pl.semaphore_signal(barrier, inc=1, device_id={"cols": lax.rem(col + k, cols)}, device_id_type=MESH)

    for dy, dx in SIDES:
        if dy:
            @pl.when(exists(dy, dx))
            def _():
                pl.semaphore_signal(barrier, inc=1, device_id={"rows": row + dy, "cols": col + dx},
                                    device_id_type=MESH)

    width = bx + 2 * PAD
    for dy in (-1, 1):
        lines = pl.ds(0, top) if dy < 0 else pl.ds(top + by, top)

        @pl.when(jnp.logical_not(exists(dy, 0)))
        def _():
            blank = jnp.zeros((top, width, 128), jnp.float32)
            for e in range(len(DEPTHS)):
                fields[e, lines] = blank
            for b in range(2):
                ping[b, lines] = blank
            fy[lines] = blank
            fx[lines] = blank
    for dx in (-1, 1):
        strip = pl.ds(0, PAD) if dx < 0 else pl.ds(PAD + bx, PAD)

        @pl.when(jnp.logical_not(exists(0, dx)))
        def _():
            @pl.loop(0, by + 2 * top)
            def _(y):
                blank = jnp.zeros((PAD, 128), jnp.float32)
                for e in range(len(DEPTHS)):
                    fields[e, y, strip] = blank
                fy[y, strip] = blank
                fx[y, strip] = blank

    def one(n, count):
        return (n + count - 1) // count

    upright = one(row, rows) + one(rows - 1 - row, rows)
    across = one(col, cols) + one(cols - 1 - col, cols)
    pl.semaphore_wait(barrier, cols - 1 + upright * (1 + across))

    def copies(e, side):
        dy, dx = SIDES[side]
        target = {"rows": row + dy, "cols": col + dx}
        corner = 1 if dy and dx else 0
        out = []
        depth = DEPTHS[e]
        jobs = [(t_hbm if e == 0 else None, fields.at[e], depth - corner)]
        if e == 0:
            jobs += [(fy_hbm, fy, top - 1 - corner), (fx_hbm, fx, top - 1 - corner)]
        for i, (src, dst, d) in enumerate(jobs):
            if d <= 0:
                continue
            ys, yd = spans(dy, d, by, top)
            xs, xd = spans(dx, d, bx, PAD)
            if src is None:
                src = fields.at[e, pl.ds(top, by), pl.ds(PAD, bx)]
            out.append(pltpu.make_async_remote_copy(
                src_ref=src.at[ys, xs], dst_ref=dst.at[yd, xd],
                send_sem=send_sem.at[e, side, i], recv_sem=recv_sem.at[e, side, i],
                device_id=target, device_id_type=MESH))
        return out

    def start(e):
        for i in range(3):
            for side, (dy, dx) in enumerate(SIDES):
                mine = copies(e, side)
                if i < len(mine):
                    @pl.when(exists(dy, dx))
                    def _():
                        mine[i].start()

    def finish(e):
        for side, (dy, dx) in enumerate(SIDES):
            @pl.when(exists(-dy, -dx))
            def _():
                for copy in copies(e, side):
                    copy.wait_recv()

    def drain(e):
        for side, (dy, dx) in enumerate(SIDES):
            @pl.when(exists(dy, dx))
            def _():
                for copy in copies(e, side):
                    copy.wait_send()

    column = lax.broadcasted_iota(jnp.int32, (1, width, 128), 1)
    keep = jnp.logical_and(
        jnp.logical_or(column >= PAD, jnp.broadcast_to(col > 0, column.shape)),
        jnp.logical_or(column < PAD + bx, jnp.broadcast_to(col < cols - 1, column.shape)))

    def update(src, y, k):
        c = src[pl.ds(y, k)]
        above, below = src[pl.ds(y + 1, k)], src[pl.ds(y - 1, k)]
        right, left = pltpu.roll(c, width - 1, 1), pltpu.roll(c, 1, 1)
        spread = (above + below) + (right + left)
        return (0.8 * c + 0.05 * spread) - fy[pl.ds(y, k)] * (above - below) - fx[pl.ds(y, k)] * (right - left)

    def advance(src, dst, margin):
        k = 2

        @pl.loop(0, by // k)
        def _(i):
            y = top + i * k
            dst[pl.ds(y, k)] = jnp.where(keep, update(src, y, k), 0.0)
        for dy in (-1, 1):
            @pl.when(exists(dy, 0))
            def _():
                y = top - margin if dy < 0 else top + by
                for j in range(margin):
                    dst[pl.ds(y + j, 1)] = jnp.where(keep, update(src, y + j, 1), 0.0)

    def advance_last(src, write):
        k = 2

        @pl.loop(0, by // k)
        def _(i):
            y = top + i * k
            write(i * k, k, update(src, y, k)[:, PAD:PAD + bx])

    start(0)
    for load in loads:
        load.wait()
    for e, depth in enumerate(DEPTHS):
        finish(e)
        src = fields.at[e]
        for s in range(depth - 1):
            dst = ping.at[s % 2]
            advance(src, dst, depth - 1 - s)
            src = dst
        if e + 1 < len(DEPTHS):
            def write(y, k, new):
                fields[e + 1, pl.ds(top + y, k), pl.ds(PAD, bx)] = new
            advance_last(src, write)
            start(e + 1)
        else:
            def write(y, k, new):
                final[pl.ds(y, k)] = new
            advance_last(src, write)

    end_copy = pltpu.make_async_copy(final, end_hbm, store_sem.at[0])
    end_copy.start()

    g = 8

    @pl.loop(0, by // g)
    def _(i):
        block = final[pl.ds(i * g, g)]
        mean = jnp.sum(block, axis=1) / bx
        off = block - mean[:, None, :]
        stats[0, pl.ds(i * g, g)] = mean
        stats[1, pl.ds(i * g, g)] = jnp.sum(off * off, axis=1)

    def share(k):
        return pltpu.make_async_remote_copy(
            src_ref=stats, dst_ref=gathered.at[k - 1],
            send_sem=stat_send.at[k - 1], recv_sem=stat_recv.at[k - 1],
            device_id={"cols": lax.rem(col + k, cols)}, device_id_type=MESH)

    @pl.loop(1, cols)
    def _(k):
        share(k).start()

    @pl.loop(1, cols)
    def _(k):
        share(k).wait_recv()

    @pl.loop(0, by // g)
    def _(i):
        lines = pl.ds(i * g, g)
        mean0 = stats[0, lines]
        mean = lax.fori_loop(0, cols - 1, lambda j, s: s + gathered[j, 0, lines], mean0) / cols
        d0 = mean0 - mean

        def add(j, s):
            d = gathered[j, 0, lines] - mean
            return s + (gathered[j, 1, lines] + bx * (d * d))
        spread = lax.fori_loop(0, cols - 1, add, stats[1, lines] + bx * (d0 * d0))
        scale = lax.rsqrt(spread / (bx * cols) + 0.0001)
        scaled[lines] = (final[lines] - mean[:, None, :]) * scale[:, None, :]

    scaled_copy = pltpu.make_async_copy(scaled, scaled_hbm, store_sem.at[1])
    scaled_copy.start()
    for e in range(len(DEPTHS)):
        drain(e)

    @pl.loop(1, cols)
    def _(k):
        share(k).wait_send()
    end_copy.wait()
    scaled_copy.wait()


def shards(rows, cols, tracer, flow_y, flow_x):
    by, bx, species = tracer.shape
    top = max(DEPTHS)
    exchanges = len(DEPTHS)
    padded = (by + 2 * top, bx + 2 * PAD, species)
    block = jax.ShapeDtypeStruct(tracer.shape, jnp.float32)
    hbm = pl.BlockSpec(memory_space=pl.ANY)
    return pl.pallas_call(
        functools.partial(kernel, rows, cols, by, bx),
        out_shape=(block, block),
        in_specs=[hbm] * 3,
        out_specs=(hbm, hbm),
        scratch_shapes=[
            pltpu.VMEM((exchanges,) + padded, jnp.float32),
            pltpu.VMEM((2,) + padded, jnp.float32),
            pltpu.VMEM(padded, jnp.float32),
            pltpu.VMEM(padded, jnp.float32),
            pltpu.VMEM(tracer.shape, jnp.float32),
            pltpu.VMEM(tracer.shape, jnp.float32),
            pltpu.VMEM((2, by, species), jnp.float32),
            pltpu.VMEM((cols - 1, 2, by, species), jnp.float32),
            pltpu.SemaphoreType.DMA((3,)),
            pltpu.SemaphoreType.DMA((exchanges, 8, 3)),
            pltpu.SemaphoreType.DMA((exchanges, 8, 3)),
            pltpu.SemaphoreType.DMA((cols - 1,)),
            pltpu.SemaphoreType.DMA((cols - 1,)),
            pltpu.SemaphoreType.DMA((2,)),
        ],
        compiler_params=pltpu.CompilerParams(
            collective_id=0, has_side_effects=True, vmem_limit_bytes=40 * 1024 * 1024),
    )(tracer, flow_y, flow_x)


def solution(mesh):
    placed = P(("site", "rows"), "cols", None)
    return jax.shard_map(
        functools.partial(shards, mesh.shape["rows"], mesh.shape["cols"]),
        mesh=mesh,
        in_specs=(placed,) * 3,
        out_specs=(placed, placed),
        check_vma=False,
    )
```

```python
import functools

import jax
import jax.numpy as jnp
from jax import lax
from jax.experimental import pallas as pl
from jax.experimental.pallas import tpu as pltpu
from jax.sharding import PartitionSpec as P

MESH = pl.DeviceIdType.MESH
DEPTHS = (3, 3)
PAD = 8
SIDES = tuple((dy, dx) for dy in (-1, 0, 1) for dx in (-1, 0, 1) if (dy, dx) != (0, 0))


def spans(side, depth, size, first, low):
    if side == 0:
        return pl.ds(0, size), pl.ds(first, size)
    if side < 0:
        return pl.ds(0, depth), pl.ds(first + size, depth)
    return pl.ds(size - depth, depth), pl.ds(low - depth, depth)


def kernel(rows, cols, by, bx, t_hbm, fy_hbm, fx_hbm, end_hbm, lines_hbm,
           fields, ping, fy, fx, final, moments, stats, gathered,
           load_sem, send_sem, recv_sem, stat_send, stat_recv, store_sem):
    row, col = lax.axis_index("rows"), lax.axis_index("cols")
    top = max(DEPTHS)

    def exists(dy, dx):
        ok = None
        for step, here, count in ((dy, row, rows), (dx, col, cols)):
            if step:
                inside = (here > 0) if step < 0 else (here < count - 1)
                ok = inside if ok is None else jnp.logical_and(ok, inside)
        return ok

    loads = [
        pltpu.make_async_copy(t_hbm, fields.at[0, pl.ds(top, by), pl.ds(0, bx)], load_sem.at[0]),
        pltpu.make_async_copy(fy_hbm, fy.at[pl.ds(top, by), pl.ds(0, bx)], load_sem.at[1]),
        pltpu.make_async_copy(fx_hbm, fx.at[pl.ds(top, by), pl.ds(0, bx)], load_sem.at[2]),
    ]
    for load in loads:
        load.start()

    barrier = pltpu.get_barrier_semaphore()

    @pl.loop(1, cols)
    def _(k):
        pl.semaphore_signal(barrier, inc=1, device_id={"cols": lax.rem(col + k, cols)}, device_id_type=MESH)

    for dy, dx in SIDES:
        if dy:
            @pl.when(exists(dy, dx))
            def _():
                pl.semaphore_signal(barrier, inc=1, device_id={"rows": row + dy, "cols": col + dx},
                                    device_id_type=MESH)

    width = bx + PAD
    for dy in (-1, 1):
        lines = pl.ds(0, top) if dy < 0 else pl.ds(top + by, top)

        @pl.when(jnp.logical_not(exists(dy, 0)))
        def _():
            blank = jnp.zeros((top, width, 128), jnp.float32)
            for e in range(len(DEPTHS)):
                fields[e, lines] = blank
            for b in range(2):
                ping[b, lines] = blank
            fy[lines] = blank
            fx[lines] = blank
    for dx in (-1, 1):
        strip = pl.ds(width - PAD // 2, PAD // 2) if dx < 0 else pl.ds(bx, PAD // 2)

        @pl.when(jnp.logical_not(exists(0, dx)))
        def _():
            @pl.loop(0, by + 2 * top)
            def _(y):
                blank = jnp.zeros((PAD // 2, 128), jnp.float32)
                for e in range(len(DEPTHS)):
                    fields[e, y, strip] = blank
                fy[y, strip] = blank
                fx[y, strip] = blank

    def one(n, count):
        return (n + count - 1) // count

    upright = one(row, rows) + one(rows - 1 - row, rows)
    across = one(col, cols) + one(cols - 1 - col, cols)
    pl.semaphore_wait(barrier, cols - 1 + upright * (1 + across))

    def copies(e, side):
        dy, dx = SIDES[side]
        target = {"rows": row + dy, "cols": col + dx}
        corner = 1 if dy and dx else 0
        out = []
        depth = DEPTHS[e]
        jobs = [(t_hbm if e == 0 else None, fields.at[e], depth - corner)]
        if e == 0:
            jobs += [(fy_hbm, fy, top - 1 - corner), (fx_hbm, fx, top - 1 - corner)]
        for i, (src, dst, d) in enumerate(jobs):
            if d <= 0:
                continue
            ys, yd = spans(dy, d, by, top, top)
            xs, xd = spans(dx, d, bx, 0, width)
            if src is None:
                src = fields.at[e, pl.ds(top, by), pl.ds(0, bx)]
            out.append(pltpu.make_async_remote_copy(
                src_ref=src.at[ys, xs], dst_ref=dst.at[yd, xd],
                send_sem=send_sem.at[e, side, i], recv_sem=recv_sem.at[e, side, i],
                device_id=target, device_id_type=MESH))
        return out

    def start(e):
        for i in range(3):
            for side, (dy, dx) in enumerate(SIDES):
                mine = copies(e, side)
                if i < len(mine):
                    @pl.when(exists(dy, dx))
                    def _():
                        mine[i].start()

    def finish(e):
        for side, (dy, dx) in enumerate(SIDES):
            @pl.when(exists(-dy, -dx))
            def _():
                for copy in copies(e, side):
                    copy.wait_recv()

    def drain(e):
        for side, (dy, dx) in enumerate(SIDES):
            @pl.when(exists(dy, dx))
            def _():
                for copy in copies(e, side):
                    copy.wait_send()

    column = lax.broadcasted_iota(jnp.int32, (1, width, 128), 1)
    keep = jnp.logical_and(
        jnp.logical_or(column < bx + PAD // 2, jnp.broadcast_to(col > 0, column.shape)),
        jnp.logical_or(jnp.logical_or(column < bx, column >= bx + PAD // 2),
                       jnp.broadcast_to(col < cols - 1, column.shape)))

    def update(src, y, k):
        c = src[pl.ds(y, k)]
        above, below = src[pl.ds(y + 1, k)], src[pl.ds(y - 1, k)]
        right, left = pltpu.roll(c, width - 1, 1), pltpu.roll(c, 1, 1)
        spread = (above + below) + (right + left)
        return (0.8 * c + 0.05 * spread) - fy[pl.ds(y, k)] * (above - below) - fx[pl.ds(y, k)] * (right - left)

    def advance(src, dst, margin):
        k = 8

        @pl.loop(0, by // k)
        def _(i):
            y = top + i * k
            dst[pl.ds(y, k)] = jnp.where(keep, update(src, y, k), 0.0)
        for dy in (-1, 1):
            @pl.when(exists(dy, 0))
            def _():
                y = top - margin if dy < 0 else top + by
                for j in range(margin):
                    dst[pl.ds(y + j, 1)] = jnp.where(keep, update(src, y + j, 1), 0.0)

    def advance_last(src, write):
        k = 8

        @pl.loop(0, by // k)
        def _(i):
            y = top + i * k
            write(i * k, k, update(src, y, k)[:, :bx])

    start(0)
    for load in loads:
        load.wait()
    for e, depth in enumerate(DEPTHS):
        finish(e)
        src = fields.at[e]
        for s in range(depth - 1):
            dst = ping.at[s % 2]
            advance(src, dst, depth - 1 - s)
            src = dst
        if e + 1 < len(DEPTHS):
            def write(y, k, new):
                fields[e + 1, pl.ds(top + y, k), pl.ds(0, bx)] = new
            advance_last(src, write)
            start(e + 1)
        else:
            def write(y, k, new):
                final[pl.ds(y, k)] = new
            advance_last(src, write)

    end_copy = pltpu.make_async_copy(final, end_hbm, store_sem.at[0])
    end_copy.start()

    g = 8

    @pl.loop(0, by // g)
    def _(i):
        block = final[pl.ds(i * g, g)]
        mean = jnp.sum(block, axis=1) / bx
        off = block - mean[:, None, :]
        stats[0, pl.ds(i * g, g)] = mean
        stats[1, pl.ds(i * g, g)] = jnp.sum(off * off, axis=1)

    def share(k):
        return pltpu.make_async_remote_copy(
            src_ref=stats, dst_ref=gathered.at[k - 1],
            send_sem=stat_send.at[k - 1], recv_sem=stat_recv.at[k - 1],
            device_id={"cols": lax.rem(col + k, cols)}, device_id_type=MESH)

    @pl.loop(1, cols)
    def _(k):
        share(k).start()

    @pl.loop(1, cols)
    def _(k):
        share(k).wait_recv()

    @pl.loop(0, by // g)
    def _(i):
        lines = pl.ds(i * g, g)
        mean0 = stats[0, lines]
        mean = lax.fori_loop(0, cols - 1, lambda j, s: s + gathered[j, 0, lines], mean0) / cols
        d0 = mean0 - mean

        def add(j, s):
            d = gathered[j, 0, lines] - mean
            return s + (gathered[j, 1, lines] + bx * (d * d))
        spread = lax.fori_loop(0, cols - 1, add, stats[1, lines] + bx * (d0 * d0))
        moments[0, lines] = mean
        moments[1, lines] = lax.rsqrt(spread / (bx * cols) + 0.0001)

    lines_copy = pltpu.make_async_copy(moments, lines_hbm, store_sem.at[1])
    lines_copy.start()
    for e in range(len(DEPTHS)):
        drain(e)

    @pl.loop(1, cols)
    def _(k):
        share(k).wait_send()
    end_copy.wait()
    lines_copy.wait()


def scale_kernel(end_hbm, lines_hbm, scaled_out, end_out, end, lines, scaled, sem):
    by = end.shape[0]
    parts = 4
    g = by // parts

    def part(i):
        return pl.ds(i * g, g)

    head = pltpu.make_async_copy(lines_hbm, lines, sem.at[0, 0])
    head.start()
    loads = [pltpu.make_async_copy(end_hbm.at[part(i)], end.at[part(i)], sem.at[1, i]) for i in range(parts)]
    for load in loads:
        load.start()
    head.wait()
    stores = []
    for i in range(parts):
        loads[i].wait()
        store = pltpu.make_async_copy(end.at[part(i)], end_out.at[part(i)], sem.at[2, i])
        store.start()
        stores.append(store)
        scaled[part(i)] = (end[part(i)] - lines[0, part(i)][:, None, :]) * lines[1, part(i)][:, None, :]
        store = pltpu.make_async_copy(scaled.at[part(i)], scaled_out.at[part(i)], sem.at[3, i])
        store.start()
        stores.append(store)
    for store in stores:
        store.wait()


def shards(rows, cols, tracer, flow_y, flow_x):
    by, bx, species = tracer.shape
    top = max(DEPTHS)
    exchanges = len(DEPTHS)
    padded = (by + 2 * top, bx + PAD, species)
    block = jax.ShapeDtypeStruct(tracer.shape, jnp.float32)
    hbm = pl.BlockSpec(memory_space=pl.ANY)
    end, lines = pl.pallas_call(
        functools.partial(kernel, rows, cols, by, bx),
        out_shape=(block, jax.ShapeDtypeStruct((2, by, species), jnp.float32)),
        in_specs=[hbm] * 3,
        out_specs=(hbm, hbm),
        scratch_shapes=[
            pltpu.VMEM((exchanges,) + padded, jnp.float32),
            pltpu.VMEM((2,) + padded, jnp.float32),
            pltpu.VMEM(padded, jnp.float32),
            pltpu.VMEM(padded, jnp.float32),
            pltpu.VMEM(tracer.shape, jnp.float32),
            pltpu.VMEM((2, by, species), jnp.float32),
            pltpu.VMEM((2, by, species), jnp.float32),
            pltpu.VMEM((cols - 1, 2, by, species), jnp.float32),
            pltpu.SemaphoreType.DMA((3,)),
            pltpu.SemaphoreType.DMA((exchanges, 8, 3)),
            pltpu.SemaphoreType.DMA((exchanges, 8, 3)),
            pltpu.SemaphoreType.DMA((cols - 1,)),
            pltpu.SemaphoreType.DMA((cols - 1,)),
            pltpu.SemaphoreType.DMA((2,)),
        ],
        compiler_params=pltpu.CompilerParams(
            collective_id=0, has_side_effects=True, vmem_limit_bytes=67043328),
    )(tracer, flow_y, flow_x)
    return pl.pallas_call(
        scale_kernel,
        out_shape=(block, block),
        in_specs=[hbm] * 2,
        out_specs=(hbm, hbm),
        scratch_shapes=[
            pltpu.VMEM(tracer.shape, jnp.float32),
            pltpu.VMEM((2, by, species), jnp.float32),
            pltpu.VMEM(tracer.shape, jnp.float32),
            pltpu.SemaphoreType.DMA((4, 4)),
        ],
        compiler_params=pltpu.CompilerParams(vmem_limit_bytes=67043328),
    )(end, lines)


def solution(mesh):
    placed = P(("site", "rows"), "cols", None)
    return jax.shard_map(
        functools.partial(shards, mesh.shape["rows"], mesh.shape["cols"]),
        mesh=mesh,
        in_specs=(placed,) * 3,
        out_specs=(placed, placed),
        check_vma=False,
    )
```

```python
import functools

import jax
import jax.numpy as jnp
from jax import lax
from jax.experimental import pallas as pl
from jax.experimental.pallas import tpu as pltpu
from jax.sharding import PartitionSpec as P

MESH = pl.DeviceIdType.MESH
DEPTHS = (3, 3)
PAD = 8
SIDES = tuple((dy, dx) for dy in (-1, 0, 1) for dx in (-1, 0, 1) if (dy, dx) != (0, 0))


def spans(side, depth, size, first, low):
    if side == 0:
        return pl.ds(0, size), pl.ds(first, size)
    if side < 0:
        return pl.ds(0, depth), pl.ds(first + size, depth)
    return pl.ds(size - depth, depth), pl.ds(low - depth, depth)


def kernel(rows, cols, by, bx, t_hbm, fy_hbm, fx_hbm, final, moments,
           fields, ping, fy, fx, stats, gathered,
           load_sem, send_sem, recv_sem, stat_send, stat_recv):
    row, col = lax.axis_index("rows"), lax.axis_index("cols")
    top = max(DEPTHS)

    def exists(dy, dx):
        ok = None
        for step, here, count in ((dy, row, rows), (dx, col, cols)):
            if step:
                inside = (here > 0) if step < 0 else (here < count - 1)
                ok = inside if ok is None else jnp.logical_and(ok, inside)
        return ok

    loads = [
        pltpu.make_async_copy(t_hbm, fields.at[0, pl.ds(top, by), pl.ds(0, bx)], load_sem.at[0]),
        pltpu.make_async_copy(fy_hbm, fy.at[pl.ds(top, by), pl.ds(0, bx)], load_sem.at[1]),
        pltpu.make_async_copy(fx_hbm, fx.at[pl.ds(top, by), pl.ds(0, bx)], load_sem.at[2]),
    ]
    for load in loads:
        load.start()

    barrier = pltpu.get_barrier_semaphore()

    @pl.loop(1, cols)
    def _(k):
        pl.semaphore_signal(barrier, inc=1, device_id={"cols": lax.rem(col + k, cols)}, device_id_type=MESH)

    for dy, dx in SIDES:
        if dy:
            @pl.when(exists(dy, dx))
            def _():
                pl.semaphore_signal(barrier, inc=1, device_id={"rows": row + dy, "cols": col + dx},
                                    device_id_type=MESH)

    width = bx + PAD
    for dy in (-1, 1):
        lines = pl.ds(0, top) if dy < 0 else pl.ds(top + by, top)

        @pl.when(jnp.logical_not(exists(dy, 0)))
        def _():
            blank = jnp.zeros((top, width, 128), jnp.float32)
            for e in range(len(DEPTHS)):
                fields[e, lines] = blank
            for b in range(2):
                ping[b, lines] = blank
            fy[lines] = blank
            fx[lines] = blank
    for dx in (-1, 1):
        strip = pl.ds(width - PAD // 2, PAD // 2) if dx < 0 else pl.ds(bx, PAD // 2)

        @pl.when(jnp.logical_not(exists(0, dx)))
        def _():
            @pl.loop(0, by + 2 * top)
            def _(y):
                blank = jnp.zeros((PAD // 2, 128), jnp.float32)
                for e in range(len(DEPTHS)):
                    fields[e, y, strip] = blank
                fy[y, strip] = blank
                fx[y, strip] = blank

    def one(n, count):
        return (n + count - 1) // count

    upright = one(row, rows) + one(rows - 1 - row, rows)
    across = one(col, cols) + one(cols - 1 - col, cols)
    pl.semaphore_wait(barrier, cols - 1 + upright * (1 + across))

    def copies(e, side):
        dy, dx = SIDES[side]
        target = {"rows": row + dy, "cols": col + dx}
        corner = 1 if dy and dx else 0
        out = []
        depth = DEPTHS[e]
        jobs = [(t_hbm if e == 0 else None, fields.at[e], depth - corner)]
        if e == 0:
            jobs += [(fy_hbm, fy, top - 1 - corner), (fx_hbm, fx, top - 1 - corner)]
        for i, (src, dst, d) in enumerate(jobs):
            if d <= 0:
                continue
            ys, yd = spans(dy, d, by, top, top)
            xs, xd = spans(dx, d, bx, 0, width)
            if src is None:
                src = fields.at[e, pl.ds(top, by), pl.ds(0, bx)]
            out.append(pltpu.make_async_remote_copy(
                src_ref=src.at[ys, xs], dst_ref=dst.at[yd, xd],
                send_sem=send_sem.at[e, side, i], recv_sem=recv_sem.at[e, side, i],
                device_id=target, device_id_type=MESH))
        return out

    def start(e):
        for i in range(3):
            for side, (dy, dx) in enumerate(SIDES):
                mine = copies(e, side)
                if i < len(mine):
                    @pl.when(exists(dy, dx))
                    def _():
                        mine[i].start()

    def finish(e):
        for side, (dy, dx) in enumerate(SIDES):
            @pl.when(exists(-dy, -dx))
            def _():
                for copy in copies(e, side):
                    copy.wait_recv()

    def drain(e):
        for side, (dy, dx) in enumerate(SIDES):
            @pl.when(exists(dy, dx))
            def _():
                for copy in copies(e, side):
                    copy.wait_send()

    column = lax.broadcasted_iota(jnp.int32, (1, width, 128), 1)
    keep = jnp.logical_and(
        jnp.logical_or(column < bx + PAD // 2, jnp.broadcast_to(col > 0, column.shape)),
        jnp.logical_or(jnp.logical_or(column < bx, column >= bx + PAD // 2),
                       jnp.broadcast_to(col < cols - 1, column.shape)))

    def update(src, y, k):
        c = src[pl.ds(y, k)]
        above, below = src[pl.ds(y + 1, k)], src[pl.ds(y - 1, k)]
        right, left = pltpu.roll(c, width - 1, 1), pltpu.roll(c, 1, 1)
        spread = (above + below) + (right + left)
        return (0.8 * c + 0.05 * spread) - fy[pl.ds(y, k)] * (above - below) - fx[pl.ds(y, k)] * (right - left)

    def advance(src, dst, margin):
        k = 8

        @pl.loop(0, by // k)
        def _(i):
            y = top + i * k
            dst[pl.ds(y, k)] = jnp.where(keep, update(src, y, k), 0.0)
        for dy in (-1, 1):
            @pl.when(exists(dy, 0))
            def _():
                y = top - margin if dy < 0 else top + by
                for j in range(margin):
                    dst[pl.ds(y + j, 1)] = jnp.where(keep, update(src, y + j, 1), 0.0)

    def advance_last(src, write):
        k = 8

        @pl.loop(0, by // k)
        def _(i):
            y = top + i * k
            write(i * k, k, update(src, y, k)[:, :bx])

    start(0)
    for load in loads:
        load.wait()
    for e, depth in enumerate(DEPTHS):
        finish(e)
        src = fields.at[e]
        for s in range(depth - 1):
            dst = ping.at[s % 2]
            advance(src, dst, depth - 1 - s)
            src = dst
        if e + 1 < len(DEPTHS):
            def write(y, k, new):
                fields[e + 1, pl.ds(top + y, k), pl.ds(0, bx)] = new
            advance_last(src, write)
            start(e + 1)
        else:
            def write(y, k, new):
                final[pl.ds(y, k)] = new
            advance_last(src, write)

    g = 8

    @pl.loop(0, by // g)
    def _(i):
        block = final[pl.ds(i * g, g)]
        mean = jnp.sum(block, axis=1) / bx
        off = block - mean[:, None, :]
        stats[0, pl.ds(i * g, g)] = mean
        stats[1, pl.ds(i * g, g)] = jnp.sum(off * off, axis=1)

    def share(k):
        return pltpu.make_async_remote_copy(
            src_ref=stats, dst_ref=gathered.at[k - 1],
            send_sem=stat_send.at[k - 1], recv_sem=stat_recv.at[k - 1],
            device_id={"cols": lax.rem(col + k, cols)}, device_id_type=MESH)

    @pl.loop(1, cols)
    def _(k):
        share(k).start()

    @pl.loop(1, cols)
    def _(k):
        share(k).wait_recv()

    @pl.loop(0, by // g)
    def _(i):
        lines = pl.ds(i * g, g)
        mean0 = stats[0, lines]
        mean = lax.fori_loop(0, cols - 1, lambda j, s: s + gathered[j, 0, lines], mean0) / cols
        d0 = mean0 - mean

        def add(j, s):
            d = gathered[j, 0, lines] - mean
            return s + (gathered[j, 1, lines] + bx * (d * d))
        spread = lax.fori_loop(0, cols - 1, add, stats[1, lines] + bx * (d0 * d0))
        moments[0, lines] = mean
        moments[1, lines] = lax.rsqrt(spread / (bx * cols) + 0.0001)
    for e in range(len(DEPTHS)):
        drain(e)

    @pl.loop(1, cols)
    def _(k):
        share(k).wait_send()


def scale_kernel(end, lines, scaled_out, end_out, scaled, sem):
    parts = 4
    g = end.shape[0] // parts
    whole = pltpu.make_async_copy(end, end_out, sem.at[parts])
    stores = [whole]
    for i in range(parts):
        part = pl.ds(i * g, g)
        scaled[part] = (end[part] - lines[0, part][:, None, :]) * lines[1, part][:, None, :]
        store = pltpu.make_async_copy(scaled.at[part], scaled_out.at[part], sem.at[i])
        store.start()
        stores.append(store)
        if i == 0:
            whole.start()
    for store in stores:
        store.wait()


def shards(rows, cols, tracer, flow_y, flow_x):
    by, bx, species = tracer.shape
    top = max(DEPTHS)
    exchanges = len(DEPTHS)
    padded = (by + 2 * top, bx + PAD, species)
    block = jax.ShapeDtypeStruct(tracer.shape, jnp.float32)
    hbm = pl.BlockSpec(memory_space=pl.ANY)
    end, lines = pl.pallas_call(
        functools.partial(kernel, rows, cols, by, bx),
        out_shape=(pltpu.VMEM(tracer.shape, jnp.float32), pltpu.VMEM((2, by, species), jnp.float32)),
        in_specs=[pl.BlockSpec(memory_space=pltpu.HBM)] * 3,
        out_specs=(pl.BlockSpec(memory_space=pltpu.VMEM),) * 2,
        scratch_shapes=[
            pltpu.VMEM((exchanges,) + padded, jnp.float32),
            pltpu.VMEM((2,) + padded, jnp.float32),
            pltpu.VMEM(padded, jnp.float32),
            pltpu.VMEM(padded, jnp.float32),
            pltpu.VMEM((2, by, species), jnp.float32),
            pltpu.VMEM((cols - 1, 2, by, species), jnp.float32),
            pltpu.SemaphoreType.DMA((3,)),
            pltpu.SemaphoreType.DMA((exchanges, 8, 3)),
            pltpu.SemaphoreType.DMA((exchanges, 8, 3)),
            pltpu.SemaphoreType.DMA((cols - 1,)),
            pltpu.SemaphoreType.DMA((cols - 1,)),
        ],
        compiler_params=pltpu.CompilerParams(
            collective_id=0, has_side_effects=True, vmem_limit_bytes=67043328 - 1024 * 1024),
    )(tracer, flow_y, flow_x)
    return pl.pallas_call(
        scale_kernel,
        out_shape=(block, block),
        in_specs=[pl.BlockSpec(memory_space=pltpu.VMEM)] * 2,
        out_specs=(hbm, hbm),
        scratch_shapes=[
            pltpu.VMEM(tracer.shape, jnp.float32),
            pltpu.SemaphoreType.DMA((5,)),
        ],
        compiler_params=pltpu.CompilerParams(vmem_limit_bytes=40 * 1024 * 1024),
    )(end, lines)


def solution(mesh):
    placed = P(("site", "rows"), "cols", None)
    return jax.shard_map(
        functools.partial(shards, mesh.shape["rows"], mesh.shape["cols"]),
        mesh=mesh,
        in_specs=(placed,) * 3,
        out_specs=(placed, placed),
        check_vma=False,
    )
```

```python
import functools

import jax
import jax.numpy as jnp
from jax import lax
from jax.experimental import pallas as pl
from jax.experimental.pallas import tpu as pltpu
from jax.sharding import PartitionSpec as P

MESH = pl.DeviceIdType.MESH
DEPTHS = (3, 3)
PAD = 8
SIDES = tuple((dy, dx) for dy in (-1, 0, 1) for dx in (-1, 0, 1) if (dy, dx) != (0, 0))


def spans(side, depth, size, first, low):
    if side == 0:
        return pl.ds(0, size), pl.ds(first, size)
    if side < 0:
        return pl.ds(0, depth), pl.ds(first + size, depth)
    return pl.ds(size - depth, depth), pl.ds(low - depth, depth)


def kernel(rows, cols, by, bx, t_hbm, fy_hbm, fx_hbm, final, moments,
           fields, ping, fy, fx, stats, gathered,
           load_sem, send_sem, recv_sem, stat_send, stat_recv):
    row, col = lax.axis_index("rows"), lax.axis_index("cols")
    top = max(DEPTHS)

    def exists(dy, dx):
        ok = None
        for step, here, count in ((dy, row, rows), (dx, col, cols)):
            if step:
                inside = (here > 0) if step < 0 else (here < count - 1)
                ok = inside if ok is None else jnp.logical_and(ok, inside)
        return ok

    loads = [
        pltpu.make_async_copy(t_hbm, fields.at[0, pl.ds(top, by), pl.ds(0, bx)], load_sem.at[0]),
        pltpu.make_async_copy(fy_hbm, fy.at[pl.ds(top, by), pl.ds(0, bx)], load_sem.at[1]),
        pltpu.make_async_copy(fx_hbm, fx.at[pl.ds(top, by), pl.ds(0, bx)], load_sem.at[2]),
    ]
    for load in loads:
        load.start()

    barrier = pltpu.get_barrier_semaphore()

    @pl.loop(1, cols)
    def _(k):
        pl.semaphore_signal(barrier, inc=1, device_id={"cols": lax.rem(col + k, cols)}, device_id_type=MESH)

    for dy, dx in SIDES:
        if dy:
            @pl.when(exists(dy, dx))
            def _():
                pl.semaphore_signal(barrier, inc=1, device_id={"rows": row + dy, "cols": col + dx},
                                    device_id_type=MESH)

    width = bx + PAD
    for dy in (-1, 1):
        lines = pl.ds(0, top) if dy < 0 else pl.ds(top + by, top)

        @pl.when(jnp.logical_not(exists(dy, 0)))
        def _():
            blank = jnp.zeros((top, width, 128), jnp.float32)
            for e in range(len(DEPTHS)):
                fields[e, lines] = blank
            for b in range(2):
                ping[b, lines] = blank
            fy[lines] = blank
            fx[lines] = blank
    for dx in (-1, 1):
        strip = pl.ds(width - PAD // 2, PAD // 2) if dx < 0 else pl.ds(bx, PAD // 2)

        @pl.when(jnp.logical_not(exists(0, dx)))
        def _():
            @pl.loop(0, by + 2 * top)
            def _(y):
                blank = jnp.zeros((PAD // 2, 128), jnp.float32)
                for e in range(len(DEPTHS)):
                    fields[e, y, strip] = blank
                fy[y, strip] = blank
                fx[y, strip] = blank

    def one(n, count):
        return (n + count - 1) // count

    upright = one(row, rows) + one(rows - 1 - row, rows)
    across = one(col, cols) + one(cols - 1 - col, cols)
    pl.semaphore_wait(barrier, cols - 1 + upright * (1 + across))

    def copies(e, side):
        dy, dx = SIDES[side]
        target = {"rows": row + dy, "cols": col + dx}
        corner = 1 if dy and dx else 0
        out = []
        depth = DEPTHS[e]
        jobs = [(t_hbm if e == 0 else None, fields.at[e], depth - corner)]
        if e == 0:
            jobs += [(fy_hbm, fy, top - 1 - corner), (fx_hbm, fx, top - 1 - corner)]
        for i, (src, dst, d) in enumerate(jobs):
            if d <= 0:
                continue
            ys, yd = spans(dy, d, by, top, top)
            xs, xd = spans(dx, d, bx, 0, width)
            if src is None:
                src = fields.at[e, pl.ds(top, by), pl.ds(0, bx)]
            out.append(pltpu.make_async_remote_copy(
                src_ref=src.at[ys, xs], dst_ref=dst.at[yd, xd],
                send_sem=send_sem.at[e, side, i], recv_sem=recv_sem.at[e, side, i],
                device_id=target, device_id_type=MESH))
        return out

    def start(e):
        for i in range(3):
            for side, (dy, dx) in enumerate(SIDES):
                mine = copies(e, side)
                if i < len(mine):
                    @pl.when(exists(dy, dx))
                    def _():
                        mine[i].start()

    def finish(e):
        for side, (dy, dx) in enumerate(SIDES):
            @pl.when(exists(-dy, -dx))
            def _():
                for copy in copies(e, side):
                    copy.wait_recv()

    def drain(e):
        for side, (dy, dx) in enumerate(SIDES):
            @pl.when(exists(dy, dx))
            def _():
                for copy in copies(e, side):
                    copy.wait_send()

    column = lax.broadcasted_iota(jnp.int32, (1, width, 128), 1)
    keep = jnp.logical_and(
        jnp.logical_or(column < bx + PAD // 2, jnp.broadcast_to(col > 0, column.shape)),
        jnp.logical_or(jnp.logical_or(column < bx, column >= bx + PAD // 2),
                       jnp.broadcast_to(col < cols - 1, column.shape)))

    def update(src, y, k):
        c = src[pl.ds(y, k)]
        above, below = src[pl.ds(y + 1, k)], src[pl.ds(y - 1, k)]
        right, left = pltpu.roll(c, width - 1, 1), pltpu.roll(c, 1, 1)
        spread = (above + below) + (right + left)
        return (0.8 * c + 0.05 * spread) - fy[pl.ds(y, k)] * (above - below) - fx[pl.ds(y, k)] * (right - left)

    def advance(src, dst, margin):
        k = 8

        @pl.loop(0, by // k)
        def _(i):
            y = top + i * k
            dst[pl.ds(y, k)] = jnp.where(keep, update(src, y, k), 0.0)
        for dy in (-1, 1):
            @pl.when(exists(dy, 0))
            def _():
                y = top - margin if dy < 0 else top + by
                for j in range(margin):
                    dst[pl.ds(y + j, 1)] = jnp.where(keep, update(src, y + j, 1), 0.0)

    def advance_last(src, write):
        k = 8

        @pl.loop(0, by // k)
        def _(i):
            y = top + i * k
            write(i * k, k, update(src, y, k)[:, :bx])

    start(0)
    for load in loads:
        load.wait()
    for e, depth in enumerate(DEPTHS):
        finish(e)
        src = fields.at[e]
        for s in range(depth - 1):
            dst = ping.at[s % 2]
            advance(src, dst, depth - 1 - s)
            src = dst
        if e + 1 < len(DEPTHS):
            def write(y, k, new):
                fields[e + 1, pl.ds(top + y, k), pl.ds(0, bx)] = new
            advance_last(src, write)
            start(e + 1)
        else:
            def write(y, k, new):
                final[pl.ds(y, k)] = new
            advance_last(src, write)

    g = 8

    @pl.loop(0, by // g)
    def _(i):
        block = final[pl.ds(i * g, g)]
        mean = jnp.sum(block, axis=1) / bx
        off = block - mean[:, None, :]
        stats[0, pl.ds(i * g, g)] = mean
        stats[1, pl.ds(i * g, g)] = jnp.sum(off * off, axis=1)

    def share(k):
        return pltpu.make_async_remote_copy(
            src_ref=stats, dst_ref=gathered.at[k - 1],
            send_sem=stat_send.at[k - 1], recv_sem=stat_recv.at[k - 1],
            device_id={"cols": lax.rem(col + k, cols)}, device_id_type=MESH)

    @pl.loop(1, cols)
    def _(k):
        share(k).start()

    @pl.loop(1, cols)
    def _(k):
        share(k).wait_recv()

    @pl.loop(0, by // g)
    def _(i):
        lines = pl.ds(i * g, g)
        mean0 = stats[0, lines]
        mean = (mean0 + jnp.sum(gathered[:, 0, lines], axis=0)) / cols
        d0 = mean0 - mean
        d = gathered[:, 0, lines] - mean
        spread = stats[1, lines] + bx * (d0 * d0) + jnp.sum(gathered[:, 1, lines] + bx * (d * d), axis=0)
        moments[0, lines] = mean
        moments[1, lines] = lax.rsqrt(spread / (bx * cols) + 0.0001)
    for e in range(len(DEPTHS)):
        drain(e)

    @pl.loop(1, cols)
    def _(k):
        share(k).wait_send()


def scale_kernel(end, lines, scaled_out, end_out, scaled, sem):
    parts = 4
    g = end.shape[0] // parts
    whole = pltpu.make_async_copy(end, end_out, sem.at[parts])
    stores = [whole]
    for i in range(parts):
        part = pl.ds(i * g, g)
        scaled[part] = (end[part] - lines[0, part][:, None, :]) * lines[1, part][:, None, :]
        store = pltpu.make_async_copy(scaled.at[part], scaled_out.at[part], sem.at[i])
        store.start()
        stores.append(store)
        if i == 0:
            whole.start()
    for store in stores:
        store.wait()


def shards(rows, cols, tracer, flow_y, flow_x):
    by, bx, species = tracer.shape
    top = max(DEPTHS)
    exchanges = len(DEPTHS)
    padded = (by + 2 * top, bx + PAD, species)
    block = jax.ShapeDtypeStruct(tracer.shape, jnp.float32)
    hbm = pl.BlockSpec(memory_space=pl.ANY)
    end, lines = pl.pallas_call(
        functools.partial(kernel, rows, cols, by, bx),
        out_shape=(pltpu.VMEM(tracer.shape, jnp.float32), pltpu.VMEM((2, by, species), jnp.float32)),
        in_specs=[pl.BlockSpec(memory_space=pltpu.HBM)] * 3,
        out_specs=(pl.BlockSpec(memory_space=pltpu.VMEM),) * 2,
        scratch_shapes=[
            pltpu.VMEM((exchanges,) + padded, jnp.float32),
            pltpu.VMEM((2,) + padded, jnp.float32),
            pltpu.VMEM(padded, jnp.float32),
            pltpu.VMEM(padded, jnp.float32),
            pltpu.VMEM((2, by, species), jnp.float32),
            pltpu.VMEM((cols - 1, 2, by, species), jnp.float32),
            pltpu.SemaphoreType.DMA((3,)),
            pltpu.SemaphoreType.DMA((exchanges, 8, 3)),
            pltpu.SemaphoreType.DMA((exchanges, 8, 3)),
            pltpu.SemaphoreType.DMA((cols - 1,)),
            pltpu.SemaphoreType.DMA((cols - 1,)),
        ],
        compiler_params=pltpu.CompilerParams(
            collective_id=0, has_side_effects=True, vmem_limit_bytes=67043328 - 1024 * 1024),
    )(tracer, flow_y, flow_x)
    return pl.pallas_call(
        scale_kernel,
        out_shape=(block, block),
        in_specs=[pl.BlockSpec(memory_space=pltpu.VMEM)] * 2,
        out_specs=(hbm, hbm),
        scratch_shapes=[
            pltpu.VMEM(tracer.shape, jnp.float32),
            pltpu.SemaphoreType.DMA((5,)),
        ],
        compiler_params=pltpu.CompilerParams(vmem_limit_bytes=40 * 1024 * 1024),
    )(end, lines)


def solution(mesh):
    placed = P(("site", "rows"), "cols", None)
    return jax.shard_map(
        functools.partial(shards, mesh.shape["rows"], mesh.shape["cols"]),
        mesh=mesh,
        in_specs=(placed,) * 3,
        out_specs=(placed, placed),
        check_vma=False,
    )
```
